32 devices in a mesh: dp: 4 (over y, x), expert: 4 (over z), tensor: 2 (over core).
Axes of the slice: x: 2, y: 2, z: 4, core: 2. Of those that a mesh axis runs over, the one named last changes fastest.
Arguments:
- out_grad: bfloat16 [2048, 2048], P(('dp', 'expert'), 'tensor'), may hold values from -6 to 6
- seq_ids: int32 [16, 128], P(('dp', 'expert')), may hold values from 0 to 3, never falling along the last dimension, each value on 1 to 64 neighbouring positions
- seq_weights: float32 [16, 4], P(('dp', 'expert')), may hold values from -1.5 to 1.5
- expert_ids: int32 [2048, 2], P(('dp', 'expert')), may hold values from 0 to 3, all different within a row; in each aligned block of 128 rows (0 to 127, 128 to 255, ...) at most 96 rows name the same one
- route_probs: bfloat16 [2048, 2], P(('dp', 'expert')), may hold values from 0.19921875 to 1
- down_weight: bfloat16 [4, 7168, 2048], P('expert', ('dp', 'tensor')), may hold values from -0.0625 to 0.0625
- gate_pre: bfloat16 [4, 7168, 1536], P('expert', ('dp', 'tensor')), may hold values from -6 to 6
- up_pre: bfloat16 [4, 7168, 1536], P('expert', ('dp', 'tensor')), may hold values from -6 to 6
Outputs:
- grad_gate: bfloat16 [4, 7168, 1536], P('expert', ('dp', 'tensor'))
- grad_up: bfloat16 [4, 7168, 1536], P('expert', ('dp', 'tensor'))
- grad_down: bfloat16 [4, 7168, 2048], P('expert', ('dp', 'tensor'))
- grad_probs: float32 [2048, 2], P(('dp', 'expert'))
The draws below stay inside these ranges and needn't reach their ends.
Inputs may be any that keep to these rules, and one draw needn't show every extreme that they name: `expert_ids`: the two experts of a token differ. Among the 128 tokens of one shard no expert is named more than 96 times, and in every draw some expert is named exactly 96 times by the tokens of some shard. `seq_ids`: along a shard's row the ids never fall; each of the 4 ids names 1 to 64 tokens of the row, and one names exactly 64.
All inputs are finite; a program needn't handle non-finite values.
Results may differ from the reference program's by a relative error of at most 0.0064.
Values may be sent and summed in bfloat16 or wider, within the bound.
A program may use at most 128 MiB of HBM per device.

```python
import math
import jax
import jax.numpy as jnp
import numpy as np
from jax import lax

D = 2048
FF = 7168
TOK_DEV = 128
SEQ_DEV = 4
EXPERTS = 4
SHARDS = 16
TOKENS = 2048
CAP = 96
SLOTS = 1536


def shard_levels(stream_key, dims, cuts, least, high):
    level, own = 1.0, jax.random.fold_in(stream_key, 6)
    for axis_at, shards_of in cuts:
        heights = jnp.exp(jax.random.uniform(jax.random.fold_in(own, axis_at), (shards_of,), jnp.float32, least / len(cuts), high / len(cuts)))
        level = level * jnp.repeat(heights, dims[axis_at] // shards_of).reshape([-1 if axis == axis_at else 1 for axis in range(len(dims))])
    return level


def length_profile(amount, total, reach, slope):
    loads = [(1 << 20) // math.isqrt(grade ** slope) + 1 for grade in range(2, amount + 1)]
    spare, counts = total - reach - (amount - 1), [1] * (amount - 1)
    while spare > 0:
        candidates = [i for i in range(amount - 1) if counts[i] < reach]
        mass, budget = sum([loads[i] for i in candidates]), spare
        for i in candidates:
            more = min(reach - counts[i], max(1, budget * loads[i] // mass), spare)
            counts[i] = counts[i] + more
            spare = spare - more
    return np.array([reach] + counts)


def ragged(rng, amount, total, bound, slope):
    if amount == 2:
        one = jax.random.randint(rng, (), max(1, total - bound), min(bound, total - 1) + 1)
        return jnp.stack([one, total - one])
    lengths = jnp.asarray(length_profile(amount, total, bound, slope), jnp.int32)
    pairs = (amount - 1) // 2
    giver, receiver = lengths[1:1 + 2 * pairs:2], lengths[2:2 + 2 * pairs:2]
    slack = jnp.minimum(giver - 1, bound - receiver)
    shifted = jax.random.randint(jax.random.fold_in(rng, 1), (pairs,), 0, 1 << 20) % (slack + 1)
    lengths = lengths.at[1:1 + 2 * pairs:2].set(giver - shifted).at[2:2 + 2 * pairs:2].set(receiver + shifted)
    return lengths[jax.random.permutation(jax.random.fold_in(rng, 2), amount)]


def shared_out(stream_key, own, number, rows, amount, top, limit, skew):
    ranking = jax.random.permutation(stream_key, amount)
    heavy_load, ordinary = load_shares(amount, rows * top, limit, skew, True), load_shares(amount, rows * top, limit, skew, False)
    places = jnp.arange(amount)

    def named(lengths, offset_by):
        used = int((lengths > 0).sum())
        fixed = max(1, used // 4)
        moved = fixed + (places - fixed + offset_by * (used - fixed)) % max(1, amount - fixed)
        return jnp.zeros((amount,), jnp.int32).at[ranking[jnp.where(places < fixed, places, moved)]].set(jnp.asarray(lengths, jnp.int32))

    lengths = jnp.where(number % 4 == 0, named(heavy_load, number // 4), named(ordinary, number - number // 4 - 1))
    mixed = jax.random.permutation(jax.random.fold_in(own, 3), amount)
    giver, sink = mixed[0:amount // 2 * 2:2], mixed[1:amount // 2 * 2:2]
    slack = jnp.minimum(lengths[giver] - 1, limit - lengths[sink]) // 2
    slack = jnp.where((giver == ranking[0]) | (sink == ranking[0]) | (lengths[sink] == 0), 0, jnp.maximum(slack, 0))
    moved = jax.random.randint(jax.random.fold_in(own, 4), (amount // 2,), 0, 1 << 20) % (slack + 1)
    lengths = lengths.at[giver].add(-moved).at[sink].add(moved)
    labels = jnp.searchsorted(jnp.cumsum(lengths), jnp.arange(rows * top), side="right").astype(jnp.int32)
    listing = labels.reshape(top, rows).T
    listing = listing[jax.random.permutation(jax.random.fold_in(own, 1), rows)]
    offset_by = jax.random.randint(jax.random.fold_in(own, 2), (rows, 1), 0, top)
    return jnp.take_along_axis(listing, (jnp.arange(top)[None, :] + offset_by) % top, axis=1)


def load_shares(count, total, bound, slope, full):
    loads = [(1 << 20) // math.isqrt(rank ** slope) + 1 for rank in range(1, count + 1)]
    largest = bound if full else min(bound, max(-(-total // count), total * loads[0] // sum(loads)))
    least = 1 if total - largest >= count - 1 else 0
    given, rest = [largest] + [least] * (count - 1), total - largest - least * (count - 1)
    while rest > 0:
        movable = [i for i in range(1, count) if given[i] < largest] or [i for i in range(1, count) if given[i] < bound]
        mass, left = sum([loads[i] for i in movable]), rest
        for i in movable:
            addition = min(bound - given[i], max(1, left * loads[i] // mass), rest)
            given[i] = given[i] + addition
            rest = rest - addition
    return np.array(given)


def gaussian(own_key, shape, scale, most, cuts=(), held_as=jnp.bfloat16):
    drawn = jax.random.normal(own_key, shape, jnp.float32) * scale
    if len(cuts) > 0:
        drawn = shard_levels(own_key, shape, cuts, -0.22, 0.18) * drawn
    return jnp.clip(drawn, min=-most, max=most).astype(held_as)


def setup_inputs(seed: int = 0) -> dict:
    key_list = jax.random.split(jax.random.key(seed), 9)
    out_grad = gaussian(key_list[0], (TOKENS, D), 0.5, 6.0, ((0, 16), (1, 2)))
    seq_ids = jax.vmap(lambda own: jnp.searchsorted(jnp.cumsum(ragged(own, SEQ_DEV, TOK_DEV, TOK_DEV // 2, 0)), jnp.arange(TOK_DEV), side="right"))(jax.random.split(key_list[1], SHARDS)).reshape((SHARDS, TOK_DEV)).astype(jnp.int32)
    seq_weights = jnp.clip(jax.random.uniform(key_list[2], (SHARDS, SEQ_DEV), jnp.float32, -1.5, 1.5) * shard_levels(key_list[2], (SHARDS, SEQ_DEV), ((0, 16),), -0.4, 0.0), -1.5, 1.5)
    expert_ids_keys = jax.random.split(jax.random.fold_in(key_list[3], 1), TOKENS // TOK_DEV)
    expert_ids_turns = jax.random.permutation(jax.random.fold_in(key_list[3], 3), TOKENS // TOK_DEV)
    expert_ids = jax.vmap(lambda own, number: shared_out(jax.random.fold_in(key_list[3], 2), own, number, TOK_DEV, EXPERTS, 2, CAP, 2))(expert_ids_keys, expert_ids_turns).reshape((TOKENS, 2))
    route_probs = jnp.clip(0.19921875 + 0.80078125 * jax.random.uniform(key_list[4], (TOKENS, 2), jnp.float32) ** shard_levels(key_list[4], (TOKENS, 2), ((0, 16),), -0.2, 0.2), 0.19921875, 1.0).astype(jnp.bfloat16)
    down_weight = gaussian(key_list[5], (EXPERTS, FF, D), FF ** -0.5, 0.0625, ((0, 4), (1, 8)))
    gate_pre = gaussian(key_list[6], (EXPERTS, FF, SLOTS), 1.0, 6.0, ((0, 4), (1, 8)))
    up_pre = gaussian(key_list[7], (EXPERTS, FF, SLOTS), 1.0, 6.0, ((0, 4), (1, 8)))
    return {"out_grad": out_grad, "seq_ids": seq_ids, "seq_weights": seq_weights, "expert_ids": expert_ids, "route_probs": route_probs, "down_weight": down_weight, "gate_pre": gate_pre, "up_pre": up_pre}


def silu_parts(pre_act):
    logistic = jax.nn.sigmoid(pre_act)
    return pre_act * logistic, logistic * (1.0 + pre_act * (1.0 - logistic))


def reference(out_grad, seq_ids, seq_weights, expert_ids, route_probs, down_weight, gate_pre, up_pre):
    shards = seq_ids.shape[0]
    token_count = seq_ids.shape[1]
    experts = down_weight.shape[0]
    capacity = gate_pre.shape[2] // shards
    feature_width = out_grad.shape[1]
    weight_tok = jnp.take_along_axis(seq_weights, seq_ids, axis=1).reshape(-1)
    scaled = (weight_tok[:, None] * out_grad.astype(jnp.float32)).astype(jnp.bfloat16)
    chosen = expert_ids.reshape(shards, 2 * token_count)
    onehot = (chosen[:, :, None] == jnp.arange(experts, dtype=jnp.int32)[None, None, :]).astype(jnp.int32)
    earlier = (jnp.cumsum(onehot, axis=1) - onehot).astype(jnp.int32)
    position = jnp.sum(earlier * onehot, axis=2).astype(jnp.int32)
    slot_index = (jnp.arange(shards, dtype=jnp.int32)[:, None] * capacity + position).reshape(-1).astype(jnp.int32)
    chosen_flat = chosen.reshape(-1).astype(jnp.int32)
    pair_rows = jnp.repeat(scaled, 2, axis=0)
    prob_flat = route_probs.reshape(-1)
    row_table = jnp.zeros((experts, shards * capacity, feature_width), jnp.bfloat16).at[chosen_flat, slot_index].set(pair_rows)
    prob_table = jnp.zeros((experts, shards * capacity), jnp.bfloat16).at[chosen_flat, slot_index].set(prob_flat)

    def per_expert(operands):
        expert_rows, expert_probs, expert_weight, gate_block, up_block = operands
        activated, derivative = silu_parts(gate_block.astype(jnp.float32))
        up_float = up_block.astype(jnp.float32)
        hidden = (activated * up_float).astype(jnp.bfloat16)
        upstream = lax.dot_general(expert_weight, expert_rows, (((1,), (1,)), ((), ())), preferred_element_type=jnp.float32)
        probe_part = jnp.sum(upstream * hidden.astype(jnp.float32), axis=0)
        factor = expert_probs.astype(jnp.float32)[None, :]
        grad_hidden = factor * upstream
        gate_out = (grad_hidden * up_float * derivative).astype(jnp.bfloat16)
        up_out = (grad_hidden * activated).astype(jnp.bfloat16)
        weighted = (expert_probs.astype(jnp.float32)[:, None] * expert_rows.astype(jnp.float32)).astype(jnp.bfloat16)
        down_out = jnp.dot(hidden, weighted, preferred_element_type=jnp.float32).astype(jnp.bfloat16)
        return gate_out, up_out, down_out, probe_part

    grad_gate, grad_up, grad_down, probe = lax.map(per_expert, (row_table, prob_table, down_weight, gate_pre, up_pre))
    grad_probs = probe[chosen_flat, slot_index].reshape(-1, 2)
    return grad_gate, grad_up, grad_down, grad_probs
```

```python
import functools

import jax
import jax.numpy as jnp
from jax import lax
from jax.experimental import pallas as pl
from jax.experimental.pallas import tpu as pltpu
from jax.sharding import PartitionSpec as P

MESH = pl.DeviceIdType.MESH
LANES = 128
SILU_ROWS = 16
DOWN_CHUNKS = 4


def flip(index, mask):
    bit = 1
    while bit <= mask:
        if mask & bit:
            index = index + bit * (1 - 2 * lax.rem(lax.div(index, bit), 2))
        bit *= 2
    return index


class Copies:
    def __init__(self, send_sem, recv_sem):
        self.send_sem, self.recv_sem, self.made = send_sem, recv_sem, []

    def start(self, src, dst, device):
        at = len(self.made)
        copy = pltpu.make_async_remote_copy(
            src_ref=src,
            dst_ref=dst,
            send_sem=self.send_sem.at[at],
            recv_sem=self.recv_sem.at[at],
            device_id=device,
            device_id_type=MESH,
        )
        copy.start()
        self.made.append(copy)
        return copy


def copy_count(columns, experts, cores):
    amount = (columns * experts - 1) + (experts - 1) + (columns * experts * cores - 1)
    if columns == 4:
        return amount + experts * (6 + 7 * (cores - 1))
    return amount + (columns - 1) + columns * (cores - 1)


def moe_kernel(
    columns,
    experts,
    cores,
    capacity,
    ids_ref,
    routes_ref,
    seq_ref,
    seq_weight_ref,
    grad_ref,
    weight_hbm,
    gate_hbm,
    up_hbm,
    gate_out,
    up_out,
    down_out,
    probs_out,
    gathered,
    rows_ref,
    prob_send,
    prob_in,
    weight_ref,
    gate_ref,
    up_ref,
    hidden_ref,
    gate_coef,
    up_coef,
    window_ref,
    scaled_hidden,
    acc_ref,
    part_ref,
    probe_in,
    load_sem,
    send_sem,
    recv_sem,
):
    d, e, t = lax.axis_index("dp"), lax.axis_index("expert"), lax.axis_index("tensor")
    tokens, half = grad_ref.shape
    width = half * cores
    group = experts * capacity
    units = weight_ref.shape[0]
    slots = gate_ref.shape[1]
    half_rows = group // 2
    span = -(-half_rows // LANES) * LANES
    upper = lax.div(2 * e, experts)
    loads = [
        pltpu.make_async_copy(src, dst, load_sem.at[at])
        for at, (src, dst) in enumerate(
            ((gate_hbm, gate_ref), (up_hbm, up_ref), (weight_hbm, weight_ref))
        )
    ]
    for load in loads:
        load.start()
    barrier = pltpu.get_barrier_semaphore()
    others = [
        (m, k, f)
        for m in range(columns)
        for k in range(experts)
        for f in range(cores)
        if m or k or f
    ]
    for m, k, f in others:
        pl.semaphore_signal(
            barrier, inc=1, device_id=(flip(d, m), flip(e, k), flip(t, f)), device_id_type=MESH
        )

    chosen = [ids_ref[k : k + 1, :] for k in range(2)]
    routes = [routes_ref[k : k + 1, :].astype(jnp.float32) for k in range(2)]
    row_at = lax.broadcasted_iota(jnp.int32, (tokens, tokens), 0)
    col_at = lax.broadcasted_iota(jnp.int32, (tokens, tokens), 1)
    lower = (row_at < col_at).astype(jnp.bfloat16)
    padded = -(-experts // 16) * 16
    expert_at = lax.broadcasted_iota(jnp.int32, (padded, tokens), 0)
    named = ((expert_at == chosen[0]) | (expert_at == chosen[1])).astype(jnp.float32)
    earlier = jnp.dot(named.astype(jnp.bfloat16), lower, preferred_element_type=jnp.float32)
    position = [
        jnp.sum(jnp.where(expert_at == chosen[k], earlier, 0.0), axis=0, keepdims=True).astype(
            jnp.int32
        )
        for k in range(2)
    ]
    seq_ids = seq_ref[...]
    seq_weights = seq_weight_ref[...]
    token_weight = jnp.zeros((1, tokens), jnp.float32)
    for s in range(seq_weights.shape[1]):
        token_weight = jnp.where(seq_ids == s, seq_weights[0:1, s : s + 1], token_weight)
    weight_column = jnp.sum(jnp.where(row_at == col_at, token_weight, 0.0), axis=1, keepdims=True)
    scaled = (weight_column * grad_ref[...].astype(jnp.float32)).astype(jnp.bfloat16)
    slot_at = lax.broadcasted_iota(jnp.int32, (capacity, tokens), 0)
    group_at = lax.broadcasted_iota(jnp.int32, (group, tokens), 0)
    own_base = e * capacity
    for k in range(experts):
        other = flip(e, k)
        key = jnp.where(
            chosen[0] == other, position[0], jnp.where(chosen[1] == other, position[1], -group - 1)
        )
        picks = (slot_at == key).astype(jnp.float32).astype(jnp.bfloat16)
        rows_ref[k] = jnp.dot(picks, scaled, preferred_element_type=jnp.float32).astype(
            jnp.bfloat16
        )
        route = jnp.where(
            chosen[0] == other, routes[0], jnp.where(chosen[1] == other, routes[1], 0.0)
        )
        spots = (group_at == key + own_base).astype(jnp.float32).astype(jnp.bfloat16)
        spread_route = lax.dot_general(
            jnp.broadcast_to(route, (16, tokens)).astype(jnp.bfloat16),
            spots,
            (((1,), (1,)), ((), ())),
            preferred_element_type=jnp.float32,
        )
        prob_send[k] = spread_route[0:1, :]
    pl.semaphore_wait(barrier, len(others))

    copies = Copies(send_sem, recv_sem)
    base = pl.multiple_of(t * half, half)
    mine = pl.ds(base, half)
    along, probs = [None], {}
    for m in range(columns):
        for k in range(experts):
            if m or k:
                probs[m, k] = copies.start(
                    prob_send.at[k], prob_in.at[m, k], (flip(d, m), flip(e, k), t)
                )
    crossing = [[[] for _ in range(experts)] for _ in range(columns)]

    def to_cores(m, k, src, dst):
        for f in range(1, cores):
            crossing[m][k].append(copies.start(src, dst, (d, e, flip(t, f))))

    def send_along():
        for k in range(1, experts):
            along.append(
                copies.start(rows_ref.at[k], gathered.at[d, e, :, mine], (d, flip(e, k), t))
            )

    def silu_rows(first, last):
        def step(i, carry):
            at = pl.ds(pl.multiple_of(i * SILU_ROWS, SILU_ROWS), SILU_ROWS)
            gate = gate_ref[at, :].astype(jnp.float32)
            up = up_ref[at, :].astype(jnp.float32)
            logistic = 0.5 * jnp.tanh(0.5 * gate) + 0.5
            activated = gate * logistic
            derivative = logistic + activated * (1.0 - logistic)
            hidden_ref[at, :] = (activated * up).astype(jnp.bfloat16)
            gate_coef[at, :] = (up * derivative).astype(jnp.bfloat16)
            up_coef[at, :] = activated.astype(jnp.bfloat16)
            return carry

        lax.fori_loop(first // SILU_ROWS, last // SILU_ROWS, step, 0)

    waited = set()

    def prob_row(m, ks):
        total = None
        for k in ks:
            if (m, k) in probs and (m, k) not in waited:
                probs[m, k].wait_recv()
                waited.add((m, k))
            row = prob_in[m, k]
            total = row if total is None else total + row
        return total

    probes = {}
    started = []

    def unit(m, h, final=False):
        near = range(experts // 2)
        far = range(experts // 2, experts)
        for k in far if h else near:
            for copy in crossing[m][k]:
                copy.wait_recv()
        where = flip(d, m)
        side = upper if h == 0 else 1 - upper
        start = pl.multiple_of(side * (group - span), LANES)
        cols = pl.ds(pl.multiple_of(where * group + start, LANES), span)
        prob_new = prob_row(m, far if h else near)
        prob_all = prob_new + prob_row(m, near) if h else prob_new
        part_ref[2] = prob_all
        part_ref[3] = prob_new
        prob_all = part_ref[2, :, pl.ds(start, span)]
        prob_new = part_ref[3, :, pl.ds(start, span)]
        if h == 0:
            inset = span - half_rows
            gap = pl.multiple_of((1 - side) * half_rows, 16)
            body = pl.multiple_of(side * inset, 16)
            if inset:
                window_ref[pl.ds(gap, inset), :] = jnp.zeros((inset, width), jnp.bfloat16)
            for k in range(experts // 2):
                window_ref[pl.ds(pl.multiple_of(body + k * capacity, 16), capacity), :] = gathered[
                    where, side * (experts // 2) + k
                ]
            block = window_ref[...]
        else:
            block = gathered.at[where].reshape(group, width)[pl.ds(start, span), :]
        tile = units // 2
        part = jnp.zeros((1, span), jnp.float32)
        for i in range(2):
            at = pl.ds(i * tile, tile)
            ups = lax.dot_general(
                weight_ref[at, :], block, (((1,), (1,)), ((), ())),
                preferred_element_type=jnp.float32,
            )
            hidden = hidden_ref[at, cols].astype(jnp.float32)
            part = part + jnp.sum(ups * hidden, axis=0, keepdims=True)
            scaled_hidden[at, :] = (hidden * prob_new).astype(jnp.bfloat16)
            grad_hidden = prob_all * ups
            gate_out[at, cols] = (grad_hidden * gate_coef[at, cols].astype(jnp.float32)).astype(
                jnp.bfloat16
            )
            up_out[at, cols] = (grad_hidden * up_coef[at, cols].astype(jnp.float32)).astype(
                jnp.bfloat16
            )
        part_ref[4 + m, :, pl.ds(start, span)] = part
        if h == 1:
            for k in range(experts):
                for f in range(cores):
                    if m or k or f:
                        probes[m, k, f] = copies.start(
                            part_ref.at[4 + m], probe_in.at[m, k, f], (where, flip(e, k), flip(t, f))
                        )
        first = not started
        started.append(True)
        chunk = width // DOWN_CHUNKS
        for j in range(DOWN_CHUNKS):
            at = pl.ds(j * chunk, chunk)
            if h == 0:
                lines = window_ref[:, at]
            else:
                lines = gathered.at[where].reshape(group, width)[pl.ds(start, span), at]
            out = jnp.dot(scaled_hidden[...], lines, preferred_element_type=jnp.float32)
            if not first:
                out = acc_ref[:, at] + out
            if final:
                down_out[:, at] = out.astype(jnp.bfloat16)
            else:
                acc_ref[:, at] = out

    if columns == 4:
        piece = half // 2
        cuts = [pl.ds(pl.multiple_of(base + p * piece, piece), piece) for p in range(2)]
        sent = {}

        def spread(k):
            origin = flip(e, k)
            if k > 0:
                along[k].wait_recv()
            for m, order in ((1, (0, 1)), (2, (1, 0))):
                for p in order:
                    here = gathered.at[d, origin, :, cuts[p]]
                    src = rows_ref.at[0, :, pl.ds(p * piece, piece)] if k == 0 else here
                    sent[k, m, p] = copies.start(src, here, (flip(d, m), e, t))
            whole = gathered.at[d, origin, :, mine]
            to_cores(0, k, rows_ref.at[0] if k == 0 else whole, whole)

        def forward(k):
            origin = flip(e, k)
            for m, p in ((1, 0), (2, 1)):
                sent[k, m, p].wait_recv()
                block = gathered.at[flip(d, m), origin, :, cuts[p]]
                sent[k, 3, p] = copies.start(block, block, (flip(d, 3 - m), e, t))
                to_cores(m, k, block, block)

        def second(k):
            origin = flip(e, k)
            for m, p in ((1, 1), (2, 0)):
                sent[k, m, p].wait_recv()
                block = gathered.at[flip(d, m), origin, :, cuts[p]]
                to_cores(m, k, block, block)

        def finish(k):
            for p in range(2):
                sent[k, 3, p].wait_recv()
                block = gathered.at[flip(d, 3), flip(e, k), :, cuts[p]]
                to_cores(3, k, block, block)

        rounds = units // SILU_ROWS
        cut = rounds * 5 // 8 * SILU_ROWS
        send_along()
        spread(0)
        gathered[d, e, :, mine] = rows_ref[0]
        prob_in[0, 0] = prob_send[0]
        loads[0].wait()
        loads[1].wait()
        silu_rows(0, cut)
        forward(0)
        second(0)
        for k in range(1, experts // 2):
            spread(k)
        silu_rows(cut, units)
        finish(0)
        loads[2].wait()
        unit(0, 0)
        for k in range(1, experts // 2):
            forward(k)
            second(k)
        spread(experts // 2)
        for k in range(1, experts // 2):
            finish(k)
        unit(1, 0)
        for k in range(experts // 2, experts - 1):
            if k > experts // 2:
                spread(k)
            forward(k)
        unit(2, 0)
        for k in range(experts // 2, experts - 1):
            second(k)
        spread(experts - 1)
        unit(3, 0)
        for k in range(experts // 2, experts - 1):
            finish(k)
        unit(0, 1)
        forward(experts - 1)
        second(experts - 1)
        unit(1, 1)
        finish(experts - 1)
        unit(2, 1)
        unit(3, 1, final=True)
    else:
        send_along()
        gathered[d, e, :, mine] = rows_ref[0]
        prob_in[0, 0] = prob_send[0]
        loads[0].wait()
        loads[1].wait()
        silu_rows(0, units)
        for k in range(1, experts):
            along[k].wait_recv()
        mine_group = gathered.at[d, :, :, mine]
        spreads = [
            copies.start(mine_group, mine_group, (flip(d, m), e, t)) for m in range(1, columns)
        ]
        to_cores(0, 0, mine_group, mine_group)
        loads[2].wait()
        for m in range(columns):
            if m:
                spreads[m - 1].wait_recv()
                block = gathered.at[flip(d, m), :, :, mine]
                to_cores(m, 0, block, block)
            unit(m, 0)
            unit(m, 1, final=m == columns - 1)

    probe_in[0, 0, 0] = part_ref[4]
    lines = []
    for k in range(experts):
        total = None
        for m in range(columns):
            for f in range(cores):
                if m or k or f:
                    probes[m, k, f].wait_recv()
                row = probe_in[m, k, f]
                total = row if total is None else total + row
        lines.append(total)
    lines.append(jnp.zeros((-(-experts // 8) * 8 - experts, group), jnp.float32))
    table = jnp.concatenate([line for line in lines if line.shape[0]], axis=0)
    line_at = lax.broadcasted_iota(jnp.int32, (table.shape[0], tokens), 0)
    for k in range(2):
        spots = (group_at == position[k] + own_base).astype(jnp.float32)
        found = jnp.dot(
            table, spots, preferred_element_type=jnp.float32, precision=lax.Precision.HIGHEST
        )
        line = jnp.full((1, tokens), -1, jnp.int32)
        for j in range(experts):
            line = jnp.where(chosen[k] == flip(e, j), j, line)
        probs_out[k : k + 1, :] = jnp.sum(
            jnp.where(line_at == line, found, 0.0), axis=0, keepdims=True
        )
    for copy in copies.made:
        copy.wait_send()


def local(out_grad, seq_ids, seq_weights, expert_ids, route_probs, down_weight, gate_pre, up_pre):
    experts = lax.axis_size("expert")
    columns = lax.axis_size("dp")
    cores = lax.axis_size("tensor")
    tokens, half = out_grad.shape
    units, slots = gate_pre.shape[1:]
    capacity = slots // (columns * experts)
    width = half * cores
    group = experts * capacity
    span = -(-(group // 2) // LANES) * LANES
    amount = copy_count(columns, experts, cores)
    anywhere = pl.BlockSpec(memory_space=pl.ANY)
    inside = pl.BlockSpec(memory_space=pltpu.VMEM)
    bf16, f32 = jnp.bfloat16, jnp.float32
    gate_grad, up_grad, down_grad, grad_probs = pl.pallas_call(
        functools.partial(moe_kernel, columns, experts, cores, capacity),
        out_shape=(
            jax.ShapeDtypeStruct((units, slots), bf16),
            jax.ShapeDtypeStruct((units, slots), bf16),
            jax.ShapeDtypeStruct((units, width), bf16),
            jax.ShapeDtypeStruct((2, tokens), f32),
        ),
        in_specs=[inside] * 5 + [anywhere] * 3,
        out_specs=[inside] * 4,
        scratch_shapes=[
            pltpu.VMEM((columns, experts, capacity, width), bf16),
            pltpu.VMEM((experts, capacity, half), bf16),
            pltpu.VMEM((experts, 1, group), f32),
            pltpu.VMEM((columns, experts, 1, group), f32),
            pltpu.VMEM((units, width), bf16),
            pltpu.VMEM((units, slots), bf16),
            pltpu.VMEM((units, slots), bf16),
            pltpu.VMEM((units, slots), bf16),
            pltpu.VMEM((units, slots), bf16),
            pltpu.VMEM((units, slots), bf16),
            pltpu.VMEM((span, width), bf16),
            pltpu.VMEM((units, span), bf16),
            pltpu.VMEM((units, width), f32),
            pltpu.VMEM((4 + columns, 1, group), f32),
            pltpu.VMEM((columns, experts, cores, 1, group), f32),
            pltpu.SemaphoreType.DMA((3,)),
            pltpu.SemaphoreType.DMA((amount,)),
            pltpu.SemaphoreType.DMA((amount,)),
        ],
        compiler_params=pltpu.CompilerParams(
            collective_id=0, has_side_effects=True, vmem_limit_bytes=VMEM_LIMIT
        ),
        name="moe",
    )(
        expert_ids.T, route_probs.T, seq_ids, seq_weights, out_grad,
        down_weight[0], gate_pre[0], up_pre[0],
    )
    return gate_grad[None], up_grad[None], down_grad[None], grad_probs.T


VMEM_LIMIT = 50 * 1024 * 1024


def solution(mesh):
    return jax.shard_map(
        local,
        mesh=mesh,
        in_specs=(
            P(("dp", "expert"), "tensor"),
            P(("dp", "expert"), None),
            P(("dp", "expert"), None),
            P(("dp", "expert"), None),
            P(("dp", "expert"), None),
            P("expert", ("dp", "tensor"), None),
            P("expert", ("dp", "tensor"), None),
            P("expert", ("dp", "tensor"), None),
        ),
        out_specs=(
            P("expert", ("dp", "tensor"), None),
            P("expert", ("dp", "tensor"), None),
            P("expert", ("dp", "tensor"), None),
            P(("dp", "expert"), None),
        ),
        check_vma=False,
    )
```

```python
import functools

import jax
import jax.numpy as jnp
from jax import lax
from jax.experimental import pallas as pl
from jax.experimental.pallas import tpu as pltpu
from jax.sharding import PartitionSpec as P

MESH = pl.DeviceIdType.MESH
LANES = 128
SILU_ROWS = 16
DOWN_CHUNKS = 4


def flip(index, mask):
    bit = 1
    while bit <= mask:
        if mask & bit:
            index = index + bit * (1 - 2 * lax.rem(lax.div(index, bit), 2))
        bit *= 2
    return index


class Copies:
    def __init__(self, send_sem, recv_sem):
        self.send_sem, self.recv_sem, self.made = send_sem, recv_sem, []

    def make(self, at, src, dst, device):
        return pltpu.make_async_remote_copy(
            src_ref=src,
            dst_ref=dst,
            send_sem=self.send_sem.at[at],
            recv_sem=self.recv_sem.at[at],
            device_id=device,
            device_id_type=MESH,
        )

    def start(self, src, dst, device):
        copy = self.make(len(self.made), src, dst, device)
        copy.start()
        self.made.append(copy)
        return copy


def copy_count(columns, experts, cores):
    amount = (columns * experts - 1) + (experts - 1) + (columns * experts * cores - 1)
    if columns == 4:
        return amount + experts * (6 + 7 * (cores - 1))
    return amount + (columns - 1) + columns * (cores - 1)


def moe_kernel(
    columns,
    experts,
    cores,
    capacity,
    ids_hbm,
    routes_hbm,
    seq_hbm,
    seq_weight_hbm,
    grad_hbm,
    weight_hbm,
    gate_hbm,
    up_hbm,
    gate_low,
    gate_high,
    up_low,
    up_high,
    down_low,
    down_high,
    probs_out,
    ids_ref,
    routes_ref,
    seq_ref,
    seq_weight_ref,
    grad_ref,
    gathered,
    rows_ref,
    prob_send,
    prob_in,
    weight_ref,
    gate_ref,
    up_ref,
    hidden_ref,
    window_ref,
    scaled_hidden,
    acc_ref,
    part_ref,
    probe_in,
    load_sem,
    send_sem,
    recv_sem,
):
    d, e, t = lax.axis_index("dp"), lax.axis_index("expert"), lax.axis_index("tensor")
    tokens, half = grad_ref.shape
    width = half * cores
    group = experts * capacity
    units = weight_ref.shape[0]
    half_rows = group // 2
    span = -(-half_rows // LANES) * LANES
    upper = lax.div(2 * e, experts)
    loads = [
        pltpu.make_async_copy(src, dst, load_sem.at[at])
        for at, (src, dst) in enumerate(
            (
                (gate_hbm, gate_ref),
                (up_hbm, up_ref),
                (weight_hbm, weight_ref),
                (ids_hbm, ids_ref),
                (routes_hbm, routes_ref),
                (seq_hbm, seq_ref),
                (seq_weight_hbm, seq_weight_ref),
                (grad_hbm, grad_ref),
            )
        )
    ]
    for load in loads[3:] + loads[:3]:
        load.start()
    barrier = pltpu.get_barrier_semaphore()
    others = [
        (m, k, f)
        for m in range(columns)
        for k in range(experts)
        for f in range(cores)
        if m or k or f
    ]
    for m, k, f in others:
        pl.semaphore_signal(
            barrier, inc=1, device_id=(flip(d, m), flip(e, k), flip(t, f)), device_id_type=MESH
        )

    for load in loads[3:]:
        load.wait()
    chosen = [ids_ref[k : k + 1, :] for k in range(2)]
    routes = [routes_ref[k : k + 1, :].astype(jnp.float32) for k in range(2)]
    row_at = lax.broadcasted_iota(jnp.int32, (tokens, tokens), 0)
    col_at = lax.broadcasted_iota(jnp.int32, (tokens, tokens), 1)
    lower = (row_at < col_at).astype(jnp.bfloat16)
    padded = -(-experts // 16) * 16
    expert_at = lax.broadcasted_iota(jnp.int32, (padded, tokens), 0)
    named = ((expert_at == chosen[0]) | (expert_at == chosen[1])).astype(jnp.float32)
    earlier = jnp.dot(named.astype(jnp.bfloat16), lower, preferred_element_type=jnp.float32)
    position = [
        jnp.sum(jnp.where(expert_at == chosen[k], earlier, 0.0), axis=0, keepdims=True).astype(
            jnp.int32
        )
        for k in range(2)
    ]
    seq_ids = seq_ref[...]
    token_weight = jnp.zeros((1, tokens), jnp.float32)
    for s in range(seq_weight_ref.shape[1]):
        token_weight = jnp.where(seq_ids == s, seq_weight_ref[0:1, s : s + 1], token_weight)
    weight_column = jnp.sum(jnp.where(row_at == col_at, token_weight, 0.0), axis=1, keepdims=True)
    scaled = (weight_column * grad_ref[...].astype(jnp.float32)).astype(jnp.bfloat16)
    slot_at = lax.broadcasted_iota(jnp.int32, (capacity, tokens), 0)
    group_at = lax.broadcasted_iota(jnp.int32, (group, tokens), 0)
    own_base = e * capacity
    for k in range(experts):
        other = flip(e, k)
        key = jnp.where(
            chosen[0] == other, position[0], jnp.where(chosen[1] == other, position[1], -group - 1)
        )
        picks = (slot_at == key).astype(jnp.float32).astype(jnp.bfloat16)
        rows_ref[k] = jnp.dot(picks, scaled, preferred_element_type=jnp.float32).astype(
            jnp.bfloat16
        )
        route = jnp.where(
            chosen[0] == other, routes[0], jnp.where(chosen[1] == other, routes[1], 0.0)
        )
        spots = (group_at == key + own_base).astype(jnp.float32).astype(jnp.bfloat16)
        spread_route = lax.dot_general(
            jnp.broadcast_to(route, (16, tokens)).astype(jnp.bfloat16),
            spots,
            (((1,), (1,)), ((), ())),
            preferred_element_type=jnp.float32,
        )
        prob_send[k] = spread_route[0:1, :]
    pl.semaphore_wait(barrier, len(others))

    copies = Copies(send_sem, recv_sem)
    base = pl.multiple_of(t * half, half)
    mine = pl.ds(base, half)
    probs = {}
    for m in range(columns):
        for k in range(experts):
            if m or k:
                probs[m, k] = copies.start(
                    prob_send.at[k], prob_in.at[m, k], (flip(d, m), flip(e, k), t)
                )
    crossing = [[[] for _ in range(experts)] for _ in range(columns)]

    def to_cores(m, k, src, dst):
        for f in range(1, cores):
            crossing[m][k].append(copies.start(src, dst, (d, e, flip(t, f))))

    first_along = len(copies.made)

    def along(k, at=None):
        place = first_along + (k if at is None else at) - 1
        return copies.make(
            place, rows_ref.at[k], gathered.at[d, e, :, mine], (d, flip(e, k), t)
        )

    for k in range(1, experts):
        copies.made.append(along(k))

    def silu_rows(first, last):
        def step(i, carry):
            at = pl.ds(pl.multiple_of(i * SILU_ROWS, SILU_ROWS), SILU_ROWS)
            gate = gate_ref[at, :].astype(jnp.float32)
            up = up_ref[at, :].astype(jnp.float32)
            logistic = 0.5 * jnp.tanh(0.5 * gate) + 0.5
            activated = gate * logistic
            derivative = logistic + activated * (1.0 - logistic)
            hidden_ref[at, :] = (activated * up).astype(jnp.bfloat16)
            gate_ref[at, :] = (up * derivative).astype(jnp.bfloat16)
            up_ref[at, :] = activated.astype(jnp.bfloat16)
            return carry

        lax.fori_loop(first // SILU_ROWS, last // SILU_ROWS, step, 0)

    waited = set()

    def prob_row(m, ks):
        total = None
        for k in ks:
            if (m, k) in probs and (m, k) not in waited:
                probs[m, k].wait_recv()
                waited.add((m, k))
            row = prob_in[m, k]
            total = row if total is None else total + row
        return total

    probes = {}
    started = []

    def arrived(m, h):
        for k in range(experts // 2 * h, experts // 2 * (h + 1)) if columns == 4 else range(1):
            for copy in crossing[m][k]:
                copy.wait_recv()
            crossing[m][k] = []

    def unit(m, h):
        with jax.named_scope(f"unit{m}{h}"):
            arrived(m, h)
            unit_down([unit_up(m, h, 0)])

    def unit_up(m, h, place):
        near = range(experts // 2)
        far = range(experts // 2, experts)
        where = flip(d, m)
        side = upper if h == 0 else 1 - upper
        start = pl.multiple_of(side * (group - span), LANES)
        cols = pl.ds(pl.multiple_of(where * group + start, LANES), span)
        prob_new = prob_row(m, far if h else near)
        prob_all = prob_new + prob_row(m, near) if h else prob_new
        part_ref[2] = prob_all
        part_ref[3] = prob_new
        prob_all = part_ref[2, :, pl.ds(start, span)]
        prob_new = part_ref[3, :, pl.ds(start, span)]
        if h == 0:
            inset = span - half_rows
            gap = pl.multiple_of((1 - side) * half_rows, 16)
            body = pl.multiple_of(side * inset, 16)
            if inset:
                window_ref[pl.ds(gap, inset), :] = jnp.zeros((inset, width), jnp.bfloat16)
            for k in range(experts // 2):
                window_ref[pl.ds(pl.multiple_of(body + k * capacity, 16), capacity), :] = gathered[
                    where, side * (experts // 2) + k
                ]
            block = window_ref[...]
        else:
            block = gathered.at[where].reshape(group, width)[pl.ds(start, span), :]
        tile = units // 2
        part = jnp.zeros((1, span), jnp.float32)
        for i in range(2):
            at = pl.ds(i * tile, tile)
            ups = lax.dot_general(
                weight_ref[at, :], block, (((1,), (1,)), ((), ())),
                preferred_element_type=jnp.float32,
            )
            hidden = hidden_ref[at, cols].astype(jnp.float32)
            part = part + jnp.sum(ups * hidden, axis=0, keepdims=True)
            scaled_hidden[place, at, :] = (hidden * prob_new).astype(jnp.bfloat16)
            grad_hidden = prob_all * ups
            (gate_low, gate_high)[i][:, cols] = (grad_hidden * gate_ref[at, cols].astype(jnp.float32)).astype(
                jnp.bfloat16
            )
            (up_low, up_high)[i][:, cols] = (grad_hidden * up_ref[at, cols].astype(jnp.float32)).astype(
                jnp.bfloat16
            )
        part_ref[4 + m, :, pl.ds(start, span)] = part
        if h == 1:
            for k in range(experts):
                for f in range(cores):
                    if m or k or f:
                        probes[m, k, f] = copies.start(
                            part_ref.at[4 + m], probe_in.at[m, k, f], (where, flip(e, k), flip(t, f))
                        )
        return where, start, h, place

    def unit_down(items, final=False):
        chunk = width // DOWN_CHUNKS
        tile = units // 2
        for where, start, h, place in items:
            first = not started
            started.append(True)
            for j in range(DOWN_CHUNKS):
                at = pl.ds(j * chunk, chunk)
                if h == 0:
                    lines = window_ref[:, at]
                else:
                    lines = gathered.at[where].reshape(group, width)[pl.ds(start, span), at]
                out = jnp.dot(scaled_hidden[place], lines, preferred_element_type=jnp.float32)
                if not first:
                    out = acc_ref[:, at] + out
                if final and place == items[-1][-1]:
                    down_low[:, at] = out[:tile].astype(jnp.bfloat16)
                    down_high[:, at] = out[tile:].astype(jnp.bfloat16)
                else:
                    acc_ref[:, at] = out

    if columns == 4:
        piece = half // 2
        cuts = [pl.ds(pl.multiple_of(base + p * piece, piece), piece) for p in range(2)]
        sent = {}

        middle = lax.div(e * (3 - e), 2)
        masks, origins = list(range(experts)), [flip(e, k) for k in range(experts)]
        if experts == 4:
            swap = middle * (origins[3] - origins[2])
            masks[2], masks[3] = 2 + middle, 3 - middle
            origins[2], origins[3] = origins[2] + swap, origins[3] - swap

        def spread(k):
            origin = origins[k]
            if k > 0:
                along(k, masks[k]).wait_recv()
            for m, order in ((1, (0, 1)), (2, (1, 0))):
                for p in order:
                    here = gathered.at[d, origin, :, cuts[p]]
                    src = rows_ref.at[0, :, pl.ds(p * piece, piece)] if k == 0 else here
                    sent[k, m, p] = copies.start(src, here, (flip(d, m), e, t))
            whole = gathered.at[d, origin, :, mine]
            to_cores(0, k, rows_ref.at[0] if k == 0 else whole, whole)

        def forward(k):
            origin = origins[k]
            for m, p in ((1, 0), (2, 1)):
                sent[k, m, p].wait_recv()
                block = gathered.at[flip(d, m), origin, :, cuts[p]]
                sent[k, 3, p] = copies.start(block, block, (flip(d, 3 - m), e, t))
                to_cores(m, k, block, block)

        def second(k):
            origin = origins[k]
            for m, p in ((1, 1), (2, 0)):
                sent[k, m, p].wait_recv()
                block = gathered.at[flip(d, m), origin, :, cuts[p]]
                to_cores(m, k, block, block)

        def finish(k):
            for p in range(2):
                sent[k, 3, p].wait_recv()
                block = gathered.at[flip(d, 3), origins[k], :, cuts[p]]
                to_cores(3, k, block, block)

        def send_far(place, order):
            if experts == 4:

                @pl.when(middle == place)
                def _():
                    for k in order:
                        along(k).start()

            elif place == 0:
                for k in range(2, experts):
                    along(k).start()

        near, last = experts // 2, experts - 1
        along(1).start()
        spread(0)
        send_far(1, (3, 2))
        gathered[d, e, :, mine] = rows_ref[0]
        prob_in[0, 0] = prob_send[0]
        loads[0].wait()
        loads[1].wait()
        silu_rows(0, units)
        forward(0)
        second(0)
        for k in range(1, near):
            spread(k)
        loads[2].wait()
        unit(0, 0)
        send_far(0, (3, 2))
        finish(0)
        for k in range(1, near):
            forward(k)
        for k in range(near, last):
            spread(k)
        for k in range(1, near):
            second(k)
        unit(1, 0)
        for k in range(1, near):
            finish(k)
        for k in range(near, last):
            forward(k)
        spread(last)
        unit(2, 0)
        for k in range(near, last):
            second(k)
        unit(3, 0)
        for k in range(near, last):
            finish(k)
        forward(last)
        unit(0, 1)
        second(last)
        unit(1, 1)
        finish(last)
        arrived(2, 1)
        arrived(3, 1)
        unit_down([unit_up(2, 1, 0), unit_up(3, 1, 1)], final=True)
    else:
        for k in range(1, experts):
            along(k).start()
        gathered[d, e, :, mine] = rows_ref[0]
        prob_in[0, 0] = prob_send[0]
        loads[0].wait()
        loads[1].wait()
        silu_rows(0, units)
        for k in range(1, experts):
            along(k).wait_recv()
        mine_group = gathered.at[d, :, :, mine]
        spreads = [
            copies.start(mine_group, mine_group, (flip(d, m), e, t)) for m in range(1, columns)
        ]
        to_cores(0, 0, mine_group, mine_group)
        loads[2].wait()
        for m in range(columns):
            if m:
                spreads[m - 1].wait_recv()
                block = gathered.at[flip(d, m), :, :, mine]
                to_cores(m, 0, block, block)
            unit(m, 0)
            unit_down([unit_up(m, 1, 0)], final=m == columns - 1)

    probe_in[0, 0, 0] = part_ref[4]
    lines = []
    for k in range(experts):
        total = None
        for m in range(columns):
            for f in range(cores):
                if m or k or f:
                    probes[m, k, f].wait_recv()
                row = probe_in[m, k, f]
                total = row if total is None else total + row
        lines.append(total)
    lines.append(jnp.zeros((-(-experts // 8) * 8 - experts, group), jnp.float32))
    table = jnp.concatenate([line for line in lines if line.shape[0]], axis=0)
    line_at = lax.broadcasted_iota(jnp.int32, (table.shape[0], tokens), 0)
    for k in range(2):
        spots = (group_at == position[k] + own_base).astype(jnp.float32)
        found = jnp.dot(
            table, spots, preferred_element_type=jnp.float32, precision=lax.Precision.HIGHEST
        )
        line = jnp.full((1, tokens), -1, jnp.int32)
        for j in range(experts):
            line = jnp.where(chosen[k] == flip(e, j), j, line)
        probs_out[k : k + 1, :] = jnp.sum(
            jnp.where(line_at == line, found, 0.0), axis=0, keepdims=True
        )
    for copy in copies.made:
        copy.wait_send()


def finish_kernel(*refs):
    parts, probs_ref, wholes, probs_hbm, sem = refs[:6], refs[6], refs[7:10], refs[10], refs[11]
    stores = [pltpu.make_async_copy(probs_ref, probs_hbm, sem.at[6])]
    for at, part in enumerate(parts):
        rows = part.shape[0]
        whole = wholes[at // 2].at[pl.ds(at % 2 * rows, rows), :]
        stores.append(pltpu.make_async_copy(part, whole, sem.at[at]))
    for store in stores:
        store.start()
    for store in stores:
        store.wait()


def size_of(shapes):
    total = 0
    for shape in shapes:
        elements = 1
        for extent in shape.shape:
            elements *= extent
        total += elements * jnp.dtype(shape.dtype).itemsize
    return total


def local(out_grad, seq_ids, seq_weights, expert_ids, route_probs, down_weight, gate_pre, up_pre):
    experts = lax.axis_size("expert")
    columns = lax.axis_size("dp")
    cores = lax.axis_size("tensor")
    tokens, half = out_grad.shape
    units, slots = gate_pre.shape[1:]
    capacity = slots // (columns * experts)
    width = half * cores
    group = experts * capacity
    span = -(-(group // 2) // LANES) * LANES
    amount = copy_count(columns, experts, cores)
    hbm = pl.BlockSpec(memory_space=pltpu.HBM)
    inside = pl.BlockSpec(memory_space=pltpu.VMEM)
    bf16, f32 = jnp.bfloat16, jnp.float32
    wholes = [
        jax.ShapeDtypeStruct((units, slots), bf16),
        jax.ShapeDtypeStruct((units, slots), bf16),
        jax.ShapeDtypeStruct((units, width), bf16),
    ]
    tail = [jax.ShapeDtypeStruct((2, tokens), f32)]
    results = [
        jax.ShapeDtypeStruct((units // 2, whole.shape[1]), bf16) for whole in wholes for _ in range(2)
    ] + tail
    scratch = [
        pltpu.VMEM((2, tokens), jnp.int32),
        pltpu.VMEM((2, tokens), bf16),
        pltpu.VMEM((1, tokens), jnp.int32),
        pltpu.VMEM(seq_weights.shape, f32),
        pltpu.VMEM((tokens, half), bf16),
        pltpu.VMEM((columns, experts, capacity, width), bf16),
        pltpu.VMEM((experts, capacity, half), bf16),
        pltpu.VMEM((experts, 1, group), f32),
        pltpu.VMEM((columns, experts, 1, group), f32),
        pltpu.VMEM((units, width), bf16),
        pltpu.VMEM((units, slots), bf16),
        pltpu.VMEM((units, slots), bf16),
        pltpu.VMEM((units, slots), bf16),
        pltpu.VMEM((span, width), bf16),
        pltpu.VMEM((2, units, span), bf16),
        pltpu.VMEM((units, width), f32),
        pltpu.VMEM((4 + columns, 1, group), f32),
        pltpu.VMEM((columns, experts, cores, 1, group), f32),
    ]
    passed = pl.pallas_call(
        functools.partial(moe_kernel, columns, experts, cores, capacity),
        out_shape=results,
        in_specs=[hbm] * 8,
        out_specs=[inside] * 7,
        scratch_shapes=scratch
        + [
            pltpu.SemaphoreType.DMA((8,)),
            pltpu.SemaphoreType.DMA((amount,)),
            pltpu.SemaphoreType.DMA((amount,)),
        ],
        compiler_params=pltpu.CompilerParams(
            collective_id=0,
            has_side_effects=True,
            vmem_limit_bytes=max(size_of(results + scratch) + SPARE, LEAST_GRANT),
        ),
        name="moe",
    )(
        *(
            pltpu.with_memory_space_constraint(array, pltpu.HBM)
            for array in (
                expert_ids.T, route_probs.T, seq_ids, seq_weights, out_grad,
                down_weight[0], gate_pre[0], up_pre[0],
            )
        )
    )
    gate_grad, up_grad, down_grad, grad_probs = pl.pallas_call(
        finish_kernel,
        out_shape=wholes + tail,
        in_specs=[inside] * 7,
        out_specs=[hbm] * 4,
        scratch_shapes=[pltpu.SemaphoreType.DMA((7,))],
        compiler_params=pltpu.CompilerParams(
            vmem_limit_bytes=size_of(results) + SPARE
        ),
        name="finish",
    )(*passed)
    return gate_grad[None], up_grad[None], down_grad[None], grad_probs.T


SPARE = 3 * 1024 * 1024
LEAST_GRANT = 44 * 1024 * 1024


def solution(mesh):
    return jax.shard_map(
        local,
        mesh=mesh,
        in_specs=(
            P(("dp", "expert"), "tensor"),
            P(("dp", "expert"), None),
            P(("dp", "expert"), None),
            P(("dp", "expert"), None),
            P(("dp", "expert"), None),
            P("expert", ("dp", "tensor"), None),
            P("expert", ("dp", "tensor"), None),
            P("expert", ("dp", "tensor"), None),
        ),
        out_specs=(
            P("expert", ("dp", "tensor"), None),
            P("expert", ("dp", "tensor"), None),
            P("expert", ("dp", "tensor"), None),
            P(("dp", "expert"), None),
        ),
        check_vma=False,
    )
```

```python
import functools

import jax
import jax.numpy as jnp
from jax import lax
from jax.experimental import pallas as pl
from jax.experimental.pallas import tpu as pltpu
from jax.sharding import PartitionSpec as P

MESH = pl.DeviceIdType.MESH
LANES = 128
SILU_ROWS = 16
DOWN_CHUNKS = 4


def flip(index, mask):
    bit = 1
    while bit <= mask:
        if mask & bit:
            index = index + bit * (1 - 2 * lax.rem(lax.div(index, bit), 2))
        bit *= 2
    return index


class Copies:
    def __init__(self, send_sem, recv_sem):
        self.send_sem, self.recv_sem, self.made = send_sem, recv_sem, []

    def make(self, at, src, dst, device):
        return pltpu.make_async_remote_copy(
            src_ref=src,
            dst_ref=dst,
            send_sem=self.send_sem.at[at],
            recv_sem=self.recv_sem.at[at],
            device_id=device,
            device_id_type=MESH,
        )

    def start(self, src, dst, device):
        copy = self.make(len(self.made), src, dst, device)
        copy.start()
        self.made.append(copy)
        return copy


def copy_count(columns, experts, cores):
    amount = (columns * experts - 1) + (experts - 1) + (columns * experts * cores - 1)
    if columns == 4:
        return amount + experts * (6 + 7 * (cores - 1))
    return amount + (columns - 1) + columns * (cores - 1)


def moe_kernel(
    columns,
    experts,
    cores,
    capacity,
    ids_hbm,
    routes_hbm,
    seq_hbm,
    seq_weight_hbm,
    grad_hbm,
    weight_hbm,
    gate_hbm,
    up_hbm,
    gate_low,
    gate_high,
    up_low,
    up_high,
    down_low,
    down_high,
    probs_out,
    ids_ref,
    routes_ref,
    seq_ref,
    seq_weight_ref,
    grad_ref,
    gathered,
    rows_ref,
    prob_send,
    prob_in,
    weight_ref,
    gate_ref,
    up_ref,
    hidden_ref,
    window_ref,
    scaled_hidden,
    acc_ref,
    part_ref,
    probe_in,
    load_sem,
    send_sem,
    recv_sem,
):
    d, e, t = lax.axis_index("dp"), lax.axis_index("expert"), lax.axis_index("tensor")
    tokens, half = grad_ref.shape
    width = half * cores
    group = experts * capacity
    units = weight_ref.shape[0]
    half_rows = group // 2
    span = -(-half_rows // LANES) * LANES
    upper = lax.div(2 * e, experts)
    loads = [
        pltpu.make_async_copy(src, dst, load_sem.at[at])
        for at, (src, dst) in enumerate(
            (
                (gate_hbm, gate_ref),
                (up_hbm, up_ref),
                (weight_hbm, weight_ref),
                (ids_hbm, ids_ref),
                (routes_hbm, routes_ref),
                (seq_hbm, seq_ref),
                (seq_weight_hbm, seq_weight_ref),
                (grad_hbm, grad_ref),
            )
        )
    ]
    for load in loads[3:] + loads[:3]:
        load.start()
    barrier = pltpu.get_barrier_semaphore()
    others = [
        (m, k, f)
        for m in range(columns)
        for k in range(experts)
        for f in range(cores)
        if m or k or f
    ]
    for m, k, f in others:
        pl.semaphore_signal(
            barrier, inc=1, device_id=(flip(d, m), flip(e, k), flip(t, f)), device_id_type=MESH
        )

    for load in loads[3:]:
        load.wait()
    chosen = [ids_ref[k : k + 1, :] for k in range(2)]
    routes = [routes_ref[k : k + 1, :].astype(jnp.float32) for k in range(2)]
    row_at = lax.broadcasted_iota(jnp.int32, (tokens, tokens), 0)
    col_at = lax.broadcasted_iota(jnp.int32, (tokens, tokens), 1)
    lower = (row_at < col_at).astype(jnp.bfloat16)
    padded = -(-experts // 16) * 16
    expert_at = lax.broadcasted_iota(jnp.int32, (padded, tokens), 0)
    named = ((expert_at == chosen[0]) | (expert_at == chosen[1])).astype(jnp.float32)
    earlier = jnp.dot(named.astype(jnp.bfloat16), lower, preferred_element_type=jnp.float32)
    position = [
        jnp.sum(jnp.where(expert_at == chosen[k], earlier, 0.0), axis=0, keepdims=True).astype(
            jnp.int32
        )
        for k in range(2)
    ]
    seq_ids = seq_ref[...]
    token_weight = jnp.zeros((1, tokens), jnp.float32)
    for s in range(seq_weight_ref.shape[1]):
        token_weight = jnp.where(seq_ids == s, seq_weight_ref[0:1, s : s + 1], token_weight)
    weight_column = jnp.sum(jnp.where(row_at == col_at, token_weight, 0.0), axis=1, keepdims=True)
    scaled = (weight_column * grad_ref[...].astype(jnp.float32)).astype(jnp.bfloat16)
    slot_at = lax.broadcasted_iota(jnp.int32, (capacity, tokens), 0)
    group_at = lax.broadcasted_iota(jnp.int32, (group, tokens), 0)
    own_base = e * capacity
    for k in range(experts):
        other = flip(e, k)
        key = jnp.where(
            chosen[0] == other, position[0], jnp.where(chosen[1] == other, position[1], -group - 1)
        )
        picks = (slot_at == key).astype(jnp.float32).astype(jnp.bfloat16)
        rows_ref[k] = jnp.dot(picks, scaled, preferred_element_type=jnp.float32).astype(
            jnp.bfloat16
        )
        route = jnp.where(
            chosen[0] == other, routes[0], jnp.where(chosen[1] == other, routes[1], 0.0)
        )
        spots = (group_at == key + own_base).astype(jnp.float32).astype(jnp.bfloat16)
        spread_route = lax.dot_general(
            jnp.broadcast_to(route, (16, tokens)).astype(jnp.bfloat16),
            spots,
            (((1,), (1,)), ((), ())),
            preferred_element_type=jnp.float32,
        )
        prob_send[k] = spread_route[0:1, :]
    pl.semaphore_wait(barrier, len(others))

    copies = Copies(send_sem, recv_sem)
    base = pl.multiple_of(t * half, half)
    mine = pl.ds(base, half)
    probs = {}
    for m in range(columns):
        for k in range(experts):
            if m or k:
                probs[m, k] = copies.start(
                    prob_send.at[k], prob_in.at[m, k], (flip(d, m), flip(e, k), t)
                )
    crossing = [[[] for _ in range(experts)] for _ in range(columns)]

    def to_cores(m, k, src, dst):
        for f in range(1, cores):
            crossing[m][k].append(copies.start(src, dst, (d, e, flip(t, f))))

    first_along = len(copies.made)

    def along(k, at=None):
        place = first_along + (k if at is None else at) - 1
        return copies.make(
            place, rows_ref.at[k], gathered.at[d, e, :, mine], (d, flip(e, k), t)
        )

    for k in range(1, experts):
        copies.made.append(along(k))

    def silu_rows(first, last):
        def step(i, carry):
            at = pl.ds(pl.multiple_of(i * SILU_ROWS, SILU_ROWS), SILU_ROWS)
            gate = gate_ref[at, :].astype(jnp.float32)
            up = up_ref[at, :].astype(jnp.float32)
            logistic = 0.5 * jnp.tanh(0.5 * gate) + 0.5
            activated = gate * logistic
            derivative = logistic + activated * (1.0 - logistic)
            hidden_ref[at, :] = (activated * up).astype(jnp.bfloat16)
            gate_ref[at, :] = (up * derivative).astype(jnp.bfloat16)
            up_ref[at, :] = activated.astype(jnp.bfloat16)
            return carry

        lax.fori_loop(first // SILU_ROWS, last // SILU_ROWS, step, 0)

    waited = set()

    def prob_row(m, ks):
        total = None
        for k in ks:
            if (m, k) in probs and (m, k) not in waited:
                probs[m, k].wait_recv()
                waited.add((m, k))
            row = prob_in[m, k]
            total = row if total is None else total + row
        return total

    probes = {}
    started = []

    def arrived(m, h):
        for k in range(experts // 2 * h, experts // 2 * (h + 1)) if columns == 4 else range(1):
            for copy in crossing[m][k]:
                copy.wait_recv()
            crossing[m][k] = []

    def unit(m, h):
        with jax.named_scope(f"unit{m}{h}"):
            arrived(m, h)
            unit_down([unit_up(m, h, 0)])

    def unit_up(m, h, place):
        near = range(experts // 2)
        far = range(experts // 2, experts)
        where = flip(d, m)
        side = upper if h == 0 else 1 - upper
        start = pl.multiple_of(side * (group - span), LANES)
        cols = pl.ds(pl.multiple_of(where * group + start, LANES), span)
        prob_new = prob_row(m, far if h else near)
        prob_all = prob_new + prob_row(m, near) if h else prob_new
        part_ref[2] = prob_all
        part_ref[3] = prob_new
        prob_all = part_ref[2, :, pl.ds(start, span)]
        prob_new = part_ref[3, :, pl.ds(start, span)]
        if h == 0:
            inset = span - half_rows
            gap = pl.multiple_of((1 - side) * half_rows, 16)
            body = pl.multiple_of(side * inset, 16)
            if inset:
                window_ref[pl.ds(gap, inset), :] = jnp.zeros((inset, width), jnp.bfloat16)
            for k in range(experts // 2):
                window_ref[pl.ds(pl.multiple_of(body + k * capacity, 16), capacity), :] = gathered[
                    where, side * (experts // 2) + k
                ]
            block = window_ref[...]
        else:
            block = gathered.at[where].reshape(group, width)[pl.ds(start, span), :]
        tile = units // 2
        part = jnp.zeros((1, span), jnp.float32)
        for i in range(2):
            at = pl.ds(i * tile, tile)
            ups = lax.dot_general(
                weight_ref[at, :], block, (((1,), (1,)), ((), ())),
                preferred_element_type=jnp.float32,
            )
            hidden = hidden_ref[at, cols].astype(jnp.float32)
            part = part + jnp.sum(ups * hidden, axis=0, keepdims=True)
            scaled_hidden[place, at, :] = (hidden * prob_new).astype(jnp.bfloat16)
            grad_hidden = prob_all * ups
            (gate_low, gate_high)[i][:, cols] = (grad_hidden * gate_ref[at, cols].astype(jnp.float32)).astype(
                jnp.bfloat16
            )
            (up_low, up_high)[i][:, cols] = (grad_hidden * up_ref[at, cols].astype(jnp.float32)).astype(
                jnp.bfloat16
            )
        part_ref[4 + m, :, pl.ds(start, span)] = part
        if h == 1:
            for k in range(experts):
                for f in range(cores):
                    if m or k or f:
                        probes[m, k, f] = copies.start(
                            part_ref.at[4 + m], probe_in.at[m, k, f], (where, flip(e, k), flip(t, f))
                        )
        return where, start, h, place

    def unit_down(items, final=False):
        chunk = width // DOWN_CHUNKS
        tile = units // 2
        for where, start, h, place in items:
            first = not started
            started.append(True)
            for j in range(DOWN_CHUNKS):
                at = pl.ds(j * chunk, chunk)
                if h == 0:
                    lines = window_ref[:, at]
                else:
                    lines = gathered.at[where].reshape(group, width)[pl.ds(start, span), at]
                out = jnp.dot(scaled_hidden[place], lines, preferred_element_type=jnp.float32)
                if not first:
                    out = acc_ref[:, at] + out
                if final and place == items[-1][-1]:
                    down_low[:, at] = out[:tile].astype(jnp.bfloat16)
                    down_high[:, at] = out[tile:].astype(jnp.bfloat16)
                else:
                    acc_ref[:, at] = out

    if columns == 4:
        piece = half // 2
        cuts = [pl.ds(pl.multiple_of(base + p * piece, piece), piece) for p in range(2)]
        sent = {}

        middle = lax.div(e * (3 - e), 2)
        masks, origins = list(range(experts)), [flip(e, k) for k in range(experts)]
        if experts == 4:
            swap = middle * (origins[3] - origins[2])
            masks[2], masks[3] = 2 + middle, 3 - middle
            origins[2], origins[3] = origins[2] + swap, origins[3] - swap

        def spread(k):
            origin = origins[k]
            if k > 0:
                along(k, masks[k]).wait_recv()
            for m, order in ((1, (0, 1)), (2, (1, 0))):
                for p in order:
                    here = gathered.at[d, origin, :, cuts[p]]
                    src = rows_ref.at[0, :, pl.ds(p * piece, piece)] if k == 0 else here
                    sent[k, m, p] = copies.start(src, here, (flip(d, m), e, t))
            whole = gathered.at[d, origin, :, mine]
            to_cores(0, k, rows_ref.at[0] if k == 0 else whole, whole)

        def forward(k):
            origin = origins[k]
            for m, p in ((1, 0), (2, 1)):
                sent[k, m, p].wait_recv()
                block = gathered.at[flip(d, m), origin, :, cuts[p]]
                sent[k, 3, p] = copies.start(block, block, (flip(d, 3 - m), e, t))
                to_cores(m, k, block, block)

        def second(k):
            origin = origins[k]
            for m, p in ((1, 1), (2, 0)):
                sent[k, m, p].wait_recv()
                block = gathered.at[flip(d, m), origin, :, cuts[p]]
                to_cores(m, k, block, block)

        def finish(k):
            for p in range(2):
                sent[k, 3, p].wait_recv()
                block = gathered.at[flip(d, 3), origins[k], :, cuts[p]]
                to_cores(3, k, block, block)

        def send_far(place, order):
            if experts == 4:

                @pl.when(middle == place)
                def _():
                    for k in order:
                        along(k).start()

            elif place == 0:
                for k in range(2, experts):
                    along(k).start()

        near, last = experts // 2, experts - 1
        along(1).start()
        spread(0)
        send_far(1, (3, 2))
        gathered[d, e, :, mine] = rows_ref[0]
        prob_in[0, 0] = prob_send[0]
        loads[0].wait()
        loads[1].wait()
        silu_rows(0, units)
        forward(0)
        second(0)
        for k in range(1, near):
            spread(k)
        loads[2].wait()
        arrived(0, 0)
        item = unit_up(0, 0, 0)
        send_far(0, (3, 2))
        unit_down([item])
        finish(0)
        for k in range(1, near):
            forward(k)
        for k in range(near, last):
            spread(k)
        for k in range(1, near):
            second(k)
        unit(1, 0)
        for k in range(1, near):
            finish(k)
        for k in range(near, last):
            forward(k)
        arrived(2, 0)
        item = unit_up(2, 0, 0)
        spread(last)
        unit_down([item])
        for k in range(near, last):
            second(k)
        unit(3, 0)
        for k in range(near, last):
            finish(k)
        arrived(0, 1)
        item = unit_up(0, 1, 0)
        forward(last)
        unit_down([item])
        second(last)
        unit(1, 1)
        finish(last)
        arrived(2, 1)
        item = unit_up(2, 1, 0)
        arrived(3, 1)
        unit_down([item, unit_up(3, 1, 1)], final=True)
    else:
        for k in range(1, experts):
            along(k).start()
        gathered[d, e, :, mine] = rows_ref[0]
        prob_in[0, 0] = prob_send[0]
        loads[0].wait()
        loads[1].wait()
        silu_rows(0, units)
        for k in range(1, experts):
            along(k).wait_recv()
        mine_group = gathered.at[d, :, :, mine]
        spreads = [
            copies.start(mine_group, mine_group, (flip(d, m), e, t)) for m in range(1, columns)
        ]
        to_cores(0, 0, mine_group, mine_group)
        loads[2].wait()
        for m in range(columns):
            if m:
                spreads[m - 1].wait_recv()
                block = gathered.at[flip(d, m), :, :, mine]
                to_cores(m, 0, block, block)
            unit(m, 0)
            unit_down([unit_up(m, 1, 0)], final=m == columns - 1)

    probe_in[0, 0, 0] = part_ref[4]
    lines = []
    for k in range(experts):
        total = None
        for m in range(columns):
            for f in range(cores):
                if m or k or f:
                    probes[m, k, f].wait_recv()
                row = probe_in[m, k, f]
                total = row if total is None else total + row
        lines.append(total)
    lines.append(jnp.zeros((-(-experts // 8) * 8 - experts, group), jnp.float32))
    table = jnp.concatenate([line for line in lines if line.shape[0]], axis=0)
    line_at = lax.broadcasted_iota(jnp.int32, (table.shape[0], tokens), 0)
    for k in range(2):
        spots = (group_at == position[k] + own_base).astype(jnp.float32)
        found = jnp.dot(
            table, spots, preferred_element_type=jnp.float32, precision=lax.Precision.HIGHEST
        )
        line = jnp.full((1, tokens), -1, jnp.int32)
        for j in range(experts):
            line = jnp.where(chosen[k] == flip(e, j), j, line)
        probs_out[k : k + 1, :] = jnp.sum(
            jnp.where(line_at == line, found, 0.0), axis=0, keepdims=True
        )
    for copy in copies.made:
        copy.wait_send()


def finish_kernel(*refs):
    parts, probs_ref, wholes, probs_hbm, sem = refs[:6], refs[6], refs[7:10], refs[10], refs[11]
    stores = [pltpu.make_async_copy(probs_ref, probs_hbm, sem.at[6])]
    for at, part in enumerate(parts):
        rows = part.shape[0]
        whole = wholes[at // 2].at[pl.ds(at % 2 * rows, rows), :]
        stores.append(pltpu.make_async_copy(part, whole, sem.at[at]))
    for store in stores:
        store.start()
    for store in stores:
        store.wait()


def size_of(shapes):
    total = 0
    for shape in shapes:
        elements = 1
        for extent in shape.shape:
            elements *= extent
        total += elements * jnp.dtype(shape.dtype).itemsize
    return total


def local(out_grad, seq_ids, seq_weights, expert_ids, route_probs, down_weight, gate_pre, up_pre):
    experts = lax.axis_size("expert")
    columns = lax.axis_size("dp")
    cores = lax.axis_size("tensor")
    tokens, half = out_grad.shape
    units, slots = gate_pre.shape[1:]
    capacity = slots // (columns * experts)
    width = half * cores
    group = experts * capacity
    span = -(-(group // 2) // LANES) * LANES
    amount = copy_count(columns, experts, cores)
    hbm = pl.BlockSpec(memory_space=pltpu.HBM)
    inside = pl.BlockSpec(memory_space=pltpu.VMEM)
    bf16, f32 = jnp.bfloat16, jnp.float32
    wholes = [
        jax.ShapeDtypeStruct((units, slots), bf16),
        jax.ShapeDtypeStruct((units, slots), bf16),
        jax.ShapeDtypeStruct((units, width), bf16),
    ]
    tail = [jax.ShapeDtypeStruct((2, tokens), f32)]
    results = [
        jax.ShapeDtypeStruct((units // 2, whole.shape[1]), bf16) for whole in wholes for _ in range(2)
    ] + tail
    scratch = [
        pltpu.VMEM((2, tokens), jnp.int32),
        pltpu.VMEM((2, tokens), bf16),
        pltpu.VMEM((1, tokens), jnp.int32),
        pltpu.VMEM(seq_weights.shape, f32),
        pltpu.VMEM((tokens, half), bf16),
        pltpu.VMEM((columns, experts, capacity, width), bf16),
        pltpu.VMEM((experts, capacity, half), bf16),
        pltpu.VMEM((experts, 1, group), f32),
        pltpu.VMEM((columns, experts, 1, group), f32),
        pltpu.VMEM((units, width), bf16),
        pltpu.VMEM((units, slots), bf16),
        pltpu.VMEM((units, slots), bf16),
        pltpu.VMEM((units, slots), bf16),
        pltpu.VMEM((span, width), bf16),
        pltpu.VMEM((2, units, span), bf16),
        pltpu.VMEM((units, width), f32),
        pltpu.VMEM((4 + columns, 1, group), f32),
        pltpu.VMEM((columns, experts, cores, 1, group), f32),
    ]
    passed = pl.pallas_call(
        functools.partial(moe_kernel, columns, experts, cores, capacity),
        out_shape=results,
        in_specs=[hbm] * 8,
        out_specs=[inside] * 7,
        scratch_shapes=scratch
        + [
            pltpu.SemaphoreType.DMA((8,)),
            pltpu.SemaphoreType.DMA((amount,)),
            pltpu.SemaphoreType.DMA((amount,)),
        ],
        compiler_params=pltpu.CompilerParams(
            collective_id=0,
            has_side_effects=True,
            vmem_limit_bytes=max(size_of(results + scratch) + SPARE, LEAST_GRANT),
        ),
        name="moe",
    )(
        *(
            pltpu.with_memory_space_constraint(array, pltpu.HBM)
            for array in (
                expert_ids.T, route_probs.T, seq_ids, seq_weights, out_grad,
                down_weight[0], gate_pre[0], up_pre[0],
            )
        )
    )
    gate_grad, up_grad, down_grad, grad_probs = pl.pallas_call(
        finish_kernel,
        out_shape=wholes + tail,
        in_specs=[inside] * 7,
        out_specs=[hbm] * 4,
        scratch_shapes=[pltpu.SemaphoreType.DMA((7,))],
        compiler_params=pltpu.CompilerParams(
            vmem_limit_bytes=size_of(results) + SPARE
        ),
        name="finish",
    )(*passed)
    return gate_grad[None], up_grad[None], down_grad[None], grad_probs.T


SPARE = 3 * 1024 * 1024
LEAST_GRANT = 44 * 1024 * 1024


def solution(mesh):
    return jax.shard_map(
        local,
        mesh=mesh,
        in_specs=(
            P(("dp", "expert"), "tensor"),
            P(("dp", "expert"), None),
            P(("dp", "expert"), None),
            P(("dp", "expert"), None),
            P(("dp", "expert"), None),
            P("expert", ("dp", "tensor"), None),
            P("expert", ("dp", "tensor"), None),
            P("expert", ("dp", "tensor"), None),
        ),
        out_specs=(
            P("expert", ("dp", "tensor"), None),
            P("expert", ("dp", "tensor"), None),
            P("expert", ("dp", "tensor"), None),
            P(("dp", "expert"), None),
        ),
        check_vma=False,
    )
```
